128 devices in a mesh: dp: 16 (over y, z), tensor: 8 (over x, core).
Axes of the slice: x: 4, y: 4, z: 4, core: 2. Of those that a mesh axis runs over, the one named last changes fastest.
Arguments:
- patches: bfloat16 [16384, 1280], P(('dp', 'tensor')), may hold values from -12 to 12
- ln_gain: float32 [1280], replicated, may hold values from 0.5 to 1.5
- ln_bias: float32 [1280], replicated, may hold values from -1.8 to 1.8
- fc1_weight: bfloat16 [5120, 2560], P(None, 'tensor'), may hold values from -0.078125 to 0.078125
- fc1_bias: float32 [2560], P('tensor'), may hold values from -3 to 3
- fc2_weight: bfloat16 [2560, 8192], P('tensor'), may hold values from -0.125 to 0.125
- fc2_bias: float32 [8192], replicated, may hold values from -3 to 3
- image_counts: int32 [128, 4], P(('dp', 'tensor')), may hold values from 0 to 32, as said below
- image_positions: int32 [4096], P(('dp', 'tensor')), may hold values from 0 to 16383, as said below
- text_embeds: bfloat16 [16384, 8192], P(('dp', 'tensor')), may hold values from -6 to 6
- keep_mask: int32 [16384, 8192], P(('dp', 'tensor')), may hold values 0 or 1
- norm_gain: float32 [8192], replicated, may hold values from 0.25 to 1.75
- qkv_weight: bfloat16 [8192, 10240], P('dp', 'tensor'), may hold values from -0.0625 to 0.0625
- qkv_bias: float32 [10240], P('tensor'), may hold values from -3 to 3
Outputs:
- stream: bfloat16 [16384, 8192], P(('dp', 'tensor'))
- queries: bfloat16 [16384, 8192], P('dp', 'tensor')
- keys: bfloat16 [16384, 1024], P('dp', 'tensor')
- values: bfloat16 [16384, 1024], P('dp', 'tensor')
The draws below stay inside these ranges and needn't reach their ends.
Inputs may be any that keep to these rules, and one draw needn't show every extreme that they name: `image_counts`: A multiple of 4. In a shard, the images after its first empty one are empty. The counts of one shard sum to at most 128, which one shard reaches in every draw. `image_positions`: all slots name distinct positions. Position p lies on the device of index p // 128 of dp+tensor. The slots of a shard name positions only on devices with the shard's tensor index, exactly 2 on each of them, so every such device receives 2 slots from each shard.
All inputs are finite; a program needn't handle non-finite values. No bound on the sum of `keep_mask` on one device may be relied on, other than what follows from the above.
Results may differ from the reference program's by a relative error of at most 0.0075.
Values may be sent and summed in bfloat16 or wider, within the bound.
No kernel may reach another device: no remote copies, remote signals or barrier semaphores. Data moves between devices by JAX's collectives and lax.ppermute only.
A program may use at most 128 MiB of HBM per device.

```python
import jax
import jax.numpy as jnp
from jax import lax

D = 8192
HEADS = 64
KV_HEADS = 8
HEAD_DIM = 128
VIT = 1280
MERGER_HID = 2560
IMG_DEV = 4
S_DEV = 128
M_DEV = 32
MERGE_IN = 5120
QKV = 10240
CAP = 2
TOKENS = 16384
PATCHES = 16384
N_DP = 16
N_TENSOR = 8
DEVICES = 128


def draw_image_counts(key, part):
    per_image = M_DEV // IMG_DEV
    key_live, key_sizes, key_full = jax.random.split(jax.random.fold_in(key, 11), 3)
    live_images = jax.random.randint(key_live, (DEVICES, 1), 1, IMG_DEV + 1)
    sizes = jax.random.randint(key_sizes, (DEVICES, IMG_DEV), 1, per_image + 1)
    full_shard = jax.random.randint(key_full, (), 0, DEVICES)
    image_idx = jnp.arange(IMG_DEV)[None, :]
    merged = jnp.where(image_idx < live_images, sizes, 0)
    merged = jnp.where(jnp.arange(DEVICES)[:, None] == full_shard, per_image, merged)
    return (4 * merged).astype(jnp.int32)


def draw_image_positions(key, part):
    key_source, key_target = jax.random.split(jax.random.fold_in(key, 23), 2)
    source_perm = jax.vmap(lambda one_key: jax.random.permutation(one_key, M_DEV))(jax.random.split(key_source, DEVICES))
    target_perm = jax.vmap(lambda one_key: jax.random.permutation(one_key, S_DEV))(jax.random.split(key_target, DEVICES))[:, :M_DEV]
    shard_ids = jnp.arange(DEVICES)
    shard_dp = shard_ids // N_TENSOR
    shard_tensor = shard_ids % N_TENSOR
    group_ids = jnp.arange(N_DP)
    within = jnp.arange(CAP)
    receiver = group_ids[None, :, None] * N_TENSOR + shard_tensor[:, None, None] + 0 * within[None, None, :]
    column = shard_dp[:, None, None] * CAP + within[None, None, :] + 0 * group_ids[None, :, None]
    target_row = target_perm[receiver, column]
    position = receiver * S_DEV + target_row
    out_slot = source_perm.reshape(DEVICES, N_DP, CAP)
    shard_index = jnp.broadcast_to(shard_ids[:, None, None], out_slot.shape)
    result = jnp.zeros((DEVICES, M_DEV), jnp.int32).at[shard_index, out_slot].set(position.astype(jnp.int32))
    return result.reshape(-1)


def plant(drawn, stream_key, smallest, high):
    dims = drawn.shape
    index_at = [jax.random.randint(jax.random.fold_in(stream_key, axis), (), 0, dims[axis]) for axis in range(len(dims))]
    drawn = drawn.at[tuple(index_at)].set(smallest)
    longest = dims.index(max(dims))
    index_at[longest] = (index_at[longest] + 1) % dims[longest]
    return drawn.at[tuple(index_at)].set(high)


def steps_of(own_key, dims, cuts, low, largest):
    level = 1.0
    for dim, shards_of in cuts:
        draws = jax.random.uniform(jax.random.fold_in(jax.random.fold_in(own_key, 6), dim), (shards_of,), jnp.float32, low / len(cuts), largest / len(cuts))
        level = level * jnp.repeat(jnp.exp(draws), dims[dim] // shards_of).reshape((-1,) + (1,) * (len(dims) - 1 - dim))
    return level


def normal_values(key, shape, scale, bound, cuts=(), held_as=jnp.bfloat16):
    values = scale * jax.random.normal(key, shape, jnp.float32)
    if cuts:
        values = values * steps_of(key, shape, cuts, -0.22, 0.18)
    return jnp.clip(values, -bound, bound).astype(held_as)


def setup_inputs(seed: int = 0) -> dict:
    seeds = jax.random.split(jax.random.key(seed), 15)
    return {
        "patches": normal_values(seeds[0], (PATCHES, VIT), 2.0, 12.0, ((0, 128),)),
        "ln_gain": jnp.clip(1.0 + 0.1 * jax.random.normal(seeds[1], (VIT,), jnp.float32), 0.5, 1.5),
        "ln_bias": normal_values(seeds[2], (VIT,), 0.3, 1.8, (), jnp.float32),
        "fc1_weight": normal_values(seeds[3], (MERGE_IN, MERGER_HID), MERGE_IN ** -0.5, 0.078125, ((1, 8),)),
        "fc1_bias": normal_values(seeds[4], (MERGER_HID,), 0.5, 3.0, ((0, 8),), jnp.float32),
        "fc2_weight": normal_values(seeds[5], (MERGER_HID, D), MERGER_HID ** -0.5, 0.125, ((0, 8),)),
        "fc2_bias": normal_values(seeds[6], (D,), 0.5, 3.0, (), jnp.float32),
        "image_counts": draw_image_counts(jax.random.fold_in(seeds[14], 71), 0),
        "image_positions": draw_image_positions(jax.random.fold_in(seeds[14], 71), 0),
        "text_embeds": normal_values(seeds[9], (TOKENS, D), 1.0, 6.0, ((0, 128),)),
        "keep_mask": plant((jax.random.randint(seeds[10], (TOKENS, D), 0, 10) < 9).astype(jnp.int32), jax.random.fold_in(seeds[10], 1), 0, 1),
        "norm_gain": jnp.clip(1.0 + 0.15 * jax.random.normal(seeds[11], (D,), jnp.float32), 0.25, 1.75),
        "qkv_weight": normal_values(seeds[12], (D, QKV), D ** -0.5, 0.0625, ((0, 16), (1, 8))),
        "qkv_bias": normal_values(seeds[13], (QKV,), 0.5, 3.0, ((0, 8),), jnp.float32),
    }


KEEP_SCALE = 1.0 / 0.9

def layer_norm(inputs, gain, bias):
    widened = inputs.astype(jnp.float32)
    center = lax.optimization_barrier(jnp.mean(widened, axis=-1, keepdims=True))
    spread = lax.optimization_barrier(jnp.mean((widened - center) * (widened - center), axis=-1, keepdims=True))
    return (widened - center) * lax.rsqrt(spread + 1e-06) * gain + bias

def rms_norm(inputs, gain):
    widened = inputs.astype(jnp.float32)
    inverse = lax.rsqrt(lax.optimization_barrier(jnp.mean(widened * widened, axis=-1, keepdims=True)) + 1e-06)
    return (widened * inverse * gain).astype(jnp.bfloat16)

def reference(patches, ln_gain, ln_bias, fc1_weight, fc1_bias, fc2_weight, fc2_bias, image_counts, image_positions, text_embeds, keep_mask, norm_gain, qkv_weight, qkv_bias):
    patch_normed = layer_norm(patches, ln_gain, ln_bias).astype(jnp.bfloat16)
    merged_in = patch_normed.reshape(-1, 4 * VIT)
    merger_hidden = jax.nn.gelu(jnp.dot(merged_in, fc1_weight, preferred_element_type=jnp.float32) + fc1_bias, approximate=False).astype(jnp.bfloat16)
    hid_rows = MERGER_HID // N_TENSOR
    summed = jnp.zeros((merged_in.shape[0], D), jnp.float32)
    for tensor_idx in range(N_TENSOR):
        lower = tensor_idx * hid_rows
        term = jnp.dot(merger_hidden[:, lower:lower + hid_rows], fc2_weight[lower:lower + hid_rows], preferred_element_type=jnp.float32)
        summed = summed + term.astype(jnp.bfloat16).astype(jnp.float32)
    merged_tokens = (summed + fc2_bias).astype(jnp.bfloat16)
    live_slots = lax.optimization_barrier(jnp.sum(image_counts, axis=1)) // 4
    usable = (jnp.arange(M_DEV, dtype=jnp.int32)[None, :] < live_slots[:, None]).reshape(-1)
    target = jnp.where(usable, image_positions, TOKENS).astype(jnp.int32)
    placed = text_embeds.at[target].set(merged_tokens, mode='drop')
    stream = (placed.astype(jnp.float32) * keep_mask.astype(jnp.float32) * KEEP_SCALE).astype(jnp.bfloat16)
    normed = rms_norm(stream, norm_gain)
    projected = jnp.dot(normed, qkv_weight, preferred_element_type=jnp.float32) + qkv_bias
    grouped = projected.reshape(TOKENS, KV_HEADS, -1)
    query_width = HEADS // KV_HEADS * HEAD_DIM
    queries = grouped[:, :, :query_width].reshape(TOKENS, -1).astype(jnp.bfloat16)
    keys = grouped[:, :, query_width:query_width + HEAD_DIM].reshape(TOKENS, -1).astype(jnp.bfloat16)
    values = grouped[:, :, query_width + HEAD_DIM:].reshape(TOKENS, -1).astype(jnp.bfloat16)
    return (stream, queries, keys, values)
```

```python
import jax
import jax.numpy as jnp
from jax import lax
from jax.experimental import pallas as pl
from jax.experimental.pallas import tpu as pltpu
from jax.sharding import PartitionSpec as P


HEAD_DIM = 128
KEEP_SCALE = 1.0 / 0.9
CHUNKS = 4
K_BLOCKS = 8
TILE = 256

UP = [(t, (t + 2) % 8) for t in range(8)]
DOWN = [(t, (t - 2) % 8) for t in range(8)]
ACROSS = [(t, t ^ 1) for t in range(8)]


def layer_norm(inputs, gain, bias):
    widened = inputs.astype(jnp.float32)
    center = jnp.mean(widened, axis=-1, keepdims=True)
    spread = jnp.mean((widened - center) * (widened - center), axis=-1, keepdims=True)
    return (widened - center) * lax.rsqrt(spread + 1e-06) * gain + bias


def rms_norm(inputs, gain):
    widened = inputs.astype(jnp.float32)
    inverse = lax.rsqrt(jnp.mean(widened * widened, axis=-1, keepdims=True) + 1e-06)
    return (widened * inverse * gain).astype(jnp.bfloat16)


def after(value, *others):
    return lax.optimization_barrier((value,) + others)[0]


def shift(value, perm):
    return lax.ppermute(value, "tensor", perm)


def gather_near(rows):
    return shift(rows, UP), shift(rows, DOWN)


def gather_far(rows, near):
    below, above = near
    half = rows.shape[0] // 2
    far_low = shift(below[:half], UP)
    far_high = shift(above[half:], DOWN)
    mine = jnp.concatenate([rows, below, above, far_low, far_high], axis=0)
    return mine, shift(mine, ACROSS)


def outgoing_rows(merged_in, image_counts, image_positions, rows_here, groups, tensor_devs):
    slots = image_positions.shape[0]
    live_slots = jnp.sum(image_counts) // 4
    usable = jnp.arange(slots, dtype=jnp.int32) < live_slots
    group = image_positions // (rows_here * tensor_devs)
    row = image_positions % rows_here
    mark = jnp.where(usable, row + 1, 0).astype(jnp.bfloat16)
    order = jnp.arange(slots, dtype=jnp.int32)
    earlier = (group[:, None] == group[None, :]) & (order[:, None] < order[None, :])
    out_slot = group * (slots // groups) + jnp.sum(earlier.astype(jnp.int32), axis=0)
    chooser = (out_slot[None, :] == order[:, None]).astype(jnp.bfloat16)
    payload = jnp.concatenate([merged_in, jnp.broadcast_to(mark[:, None], (slots, 128))], axis=1)
    return jnp.dot(chooser, payload, preferred_element_type=jnp.float32).astype(jnp.bfloat16)


def project_body(owners, *refs):
    pieces = refs[: 2 * CHUNKS + 2]
    weight, bias, place, hit, queries, keys, values, rows, total, done, sems = refs[2 * CHUNKS + 2 :]
    tile = pl.program_id(0)
    height, depth = pieces[0].shape
    step = depth // K_BLOCKS
    count = len(pieces)
    live = 2 * CHUNKS * height
    per_owner = height // 4

    def copy(piece, block):
        span = pl.ds(pl.multiple_of(block * step, step), step)
        return pltpu.make_async_copy(
            pieces[piece].at[:, span], rows.at[pl.ds(piece * height, height), span], sems.at[block, piece]
        )

    @pl.when(tile == 0)
    def _():
        for block in range(K_BLOCKS):
            for piece in range(count):
                copy(piece, block).start()

    total[...] = jnp.broadcast_to(bias[...], total.shape)

    def accumulate(block, carry):
        @pl.when(tile == 0)
        def _():
            for piece in range(count):
                copy(piece, block).wait()

        span = pl.ds(pl.multiple_of(block * step, step), step)
        total[...] += jnp.dot(rows[:, span], weight[span, :], preferred_element_type=jnp.float32)
        return carry

    lax.fori_loop(0, K_BLOCKS, accumulate, 0)
    tokens = total[live:, :].astype(jnp.bfloat16)

    for chunk in range(CHUNKS):
        lower = chunk * 2 * height
        part = slice(lower, lower + 2 * height)
        moved = jnp.dot(place[part, :], tokens, preferred_element_type=jnp.float32)
        done[part, :] = jnp.where(hit[part, :1] > 0.5, moved, total[part, :]).astype(jnp.bfloat16)

    def write(store):
        for chunk in range(CHUNKS):
            for owner in range(8):
                source = chunk * 2 * height + owner * per_owner
                target = pl.multiple_of(owners[owner] * (CHUNKS * per_owner) + chunk * per_owner, per_owner)
                store(source, target)

    @pl.when(tile < 4)
    def _():
        def store(source, target):
            queries[pl.ds(target, per_owner), :] = done[source : source + per_owner, :]

        write(store)

    @pl.when(tile == 4)
    def _():
        def store(source, target):
            keys[pl.ds(target, per_owner), :] = done[source : source + per_owner, :HEAD_DIM]
            values[pl.ds(target, per_owner), :] = done[source : source + per_owner, HEAD_DIM:]

        write(store)


def project(owners, pieces, weight, bias, place, hit):
    height, depth = pieces[0].shape
    total_rows = len(pieces) * height
    live = 2 * CHUNKS * height
    tiles = weight.shape[1] // TILE
    anywhere = pl.BlockSpec(memory_space=pl.ANY)
    return pl.pallas_call(
        project_body,
        name="project",
        grid_spec=pltpu.PrefetchScalarGridSpec(
            num_scalar_prefetch=1,
            grid=(tiles,),
            in_specs=[anywhere] * len(pieces)
            + [
                pl.BlockSpec((depth, TILE), lambda n, o: (0, n)),
                pl.BlockSpec((1, TILE), lambda n, o: (0, n)),
                pl.BlockSpec(place.shape, lambda n, o: (0, 0)),
                pl.BlockSpec(hit.shape, lambda n, o: (0, 0)),
            ],
            out_specs=[
                pl.BlockSpec((live, TILE), lambda n, o: (0, jnp.minimum(n, 3))),
                pl.BlockSpec((live, HEAD_DIM), lambda n, o: (0, 0)),
                pl.BlockSpec((live, HEAD_DIM), lambda n, o: (0, 0)),
            ],
            scratch_shapes=[
                pltpu.VMEM((total_rows, depth), jnp.bfloat16),
                pltpu.VMEM((total_rows, TILE), jnp.float32),
                pltpu.VMEM((live, TILE), jnp.bfloat16),
                pltpu.SemaphoreType.DMA((K_BLOCKS, len(pieces))),
            ],
        ),
        out_shape=[
            jax.ShapeDtypeStruct((live, 8 * HEAD_DIM), jnp.bfloat16),
            jax.ShapeDtypeStruct((live, HEAD_DIM), jnp.bfloat16),
            jax.ShapeDtypeStruct((live, HEAD_DIM), jnp.bfloat16),
        ],
        compiler_params=pltpu.CompilerParams(
            dimension_semantics=("arbitrary",), vmem_limit_bytes=56 * 1024 * 1024
        ),
        cost_estimate=pl.CostEstimate(
            flops=2 * total_rows * depth * weight.shape[1], bytes_accessed=50_000_000, transcendentals=0
        ),
    )(owners, *pieces, weight, bias[None, :], place, hit)


def shards(
    patches, ln_gain, ln_bias, fc1_weight, fc1_bias, fc2_weight, fc2_bias, image_counts, image_positions,
    text_embeds, keep_mask, norm_gain, qkv_weight, qkv_bias,
):
    groups = lax.axis_size("dp")
    tensor_devs = lax.axis_size("tensor")
    device = lax.axis_index("tensor")
    rows_here, _ = text_embeds.shape
    weight = lax.all_gather(qkv_weight, "dp", axis=0, tiled=True)

    patch_normed = layer_norm(patches, ln_gain, ln_bias).astype(jnp.bfloat16)
    merged_in = patch_normed.reshape(-1, 4 * patches.shape[1])
    slots, features = merged_in.shape
    outgoing = outgoing_rows(merged_in, image_counts, image_positions, rows_here, groups, tensor_devs)
    arrived = lax.all_to_all(
        outgoing.reshape(groups, slots // groups, -1), "dp", split_axis=0, concat_axis=0, tiled=True
    ).reshape(slots, -1)

    text_stream = (text_embeds.astype(jnp.float32) * keep_mask.astype(jnp.float32) * KEEP_SCALE).astype(jnp.bfloat16)
    text_normed = rms_norm(text_stream, norm_gain)
    per_chunk = rows_here // CHUNKS
    chunks = [text_normed[c * per_chunk : (c + 1) * per_chunk] for c in range(CHUNKS)]
    near0 = gather_near(chunks[0])

    mine, other = gather_far(arrived, gather_near(arrived))
    together = jnp.concatenate([mine, other], axis=0)
    far0 = gather_far(chunks[0], (after(near0[0], together), near0[1]))
    chunk1 = after(chunks[1], together)
    near1 = gather_near(chunk1)

    product = jnp.dot(together[:, :features], fc1_weight, preferred_element_type=jnp.float32) + fc1_bias
    hidden = jax.nn.gelu(product, approximate=False).astype(jnp.bfloat16)
    partial = jnp.dot(hidden, fc2_weight, preferred_element_type=jnp.float32).astype(jnp.bfloat16)
    theirs = shift(partial[4 * slots :], ACROSS)
    paired = (partial[: 4 * slots].astype(jnp.float32) + theirs.astype(jnp.float32)).astype(jnp.bfloat16)
    half = slots // 2
    low = shift(paired[3 * slots : 3 * slots + half], UP)
    high = shift(paired[3 * slots + half : 4 * slots], DOWN)
    zeros = jnp.zeros_like(low)
    to_above = paired[2 * slots : 3 * slots].astype(jnp.float32) + jnp.concatenate([low, zeros], axis=0).astype(jnp.float32)
    to_below = paired[slots : 2 * slots].astype(jnp.float32) + jnp.concatenate([zeros, high], axis=0).astype(jnp.float32)
    from_below = shift(to_above.astype(jnp.bfloat16), UP)
    from_above = shift(to_below.astype(jnp.bfloat16), DOWN)
    summed = paired[:slots].astype(jnp.float32) + from_below.astype(jnp.float32) + from_above.astype(jnp.float32)
    tokens = (summed + fc2_bias).astype(jnp.bfloat16)

    far1 = gather_far(chunk1, (after(near1[0], tokens), near1[1]))
    chunk2 = after(chunks[2], tokens)
    near2 = gather_near(chunk2)

    own_row = arrived[:, features].astype(jnp.int32) - 1
    landing = own_row[None, :] == jnp.arange(rows_here, dtype=jnp.int32)[:, None]
    covered = jnp.any(landing, axis=1)
    token_mask = lax.dot_general(
        landing.astype(jnp.bfloat16), keep_mask.astype(jnp.bfloat16), (((0,), (0,)), ((), ())),
        preferred_element_type=jnp.float32,
    )
    token_stream = (tokens.astype(jnp.float32) * token_mask * KEEP_SCALE).astype(jnp.bfloat16)
    token_normed = rms_norm(token_stream, norm_gain)
    token_all = gather_far(token_normed, gather_near(token_normed))
    far2 = gather_far(chunk2, (after(near2[0], token_all[0]), near2[1]))
    chunk3 = after(chunks[3], token_all[0])
    far3 = gather_far(chunk3, gather_near(chunk3))

    landed = jnp.dot(landing.astype(jnp.bfloat16), token_stream, preferred_element_type=jnp.float32)
    stream = jnp.where(covered[:, None], landed.astype(jnp.bfloat16), text_stream)

    slot_row = together[:, features].astype(jnp.int32) - 1
    row = jnp.arange(rows_here * tensor_devs, dtype=jnp.int32)
    row_owner = row // per_chunk % tensor_devs
    row_index = row // (per_chunk * tensor_devs) * per_chunk + row % per_chunk
    slot_owner = jnp.arange(slots * tensor_devs, dtype=jnp.int32) // slots
    place = (row_owner[:, None] == slot_owner[None, :]) & (row_index[:, None] == slot_row[None, :])
    hit = jnp.broadcast_to(jnp.any(place, axis=1)[:, None], (row.shape[0], 128)).astype(jnp.float32)
    owners = jnp.stack([(base + step) % tensor_devs for base in (device, device ^ 1) for step in (0, -2, 2, 4)])
    queries, keys, values = project(
        owners.astype(jnp.int32), [*far0, *far1, *far2, *far3, *token_all], weight, qkv_bias,
        place.astype(jnp.bfloat16), hit,
    )
    return (stream, queries, keys, values)


def solution(mesh):
    placed = (
        P(("dp", "tensor"), None), P(), P(), P(None, "tensor"), P("tensor"), P("tensor", None), P(),
        P(("dp", "tensor"), None), P(("dp", "tensor")), P(("dp", "tensor"), None), P(("dp", "tensor"), None),
        P(), P("dp", "tensor"), P("tensor"),
    )

    return jax.shard_map(
        shards, mesh=mesh, in_specs=placed,
        out_specs=(P(("dp", "tensor"), None), P("dp", "tensor"), P("dp", "tensor"), P("dp", "tensor")),
        check_vma=False,
    )
```

```python
import jax
import jax.numpy as jnp
from jax import lax
from jax.experimental import pallas as pl
from jax.experimental.pallas import tpu as pltpu
from jax.sharding import PartitionSpec as P


HEAD_DIM = 128
KEEP_SCALE = 1.0 / 0.9
K_BLOCKS = 8

UP = [(t, (t + 2) % 8) for t in range(8)]
DOWN = [(t, (t - 2) % 8) for t in range(8)]
ACROSS = [(t, t ^ 1) for t in range(8)]


def layer_norm(inputs, gain, bias):
    widened = inputs.astype(jnp.float32)
    center = jnp.mean(widened, axis=-1, keepdims=True)
    spread = jnp.mean((widened - center) * (widened - center), axis=-1, keepdims=True)
    return (widened - center) * lax.rsqrt(spread + 1e-06) * gain + bias


def rms_norm(inputs, gain):
    widened = inputs.astype(jnp.float32)
    inverse = lax.rsqrt(jnp.mean(widened * widened, axis=-1, keepdims=True) + 1e-06)
    return (widened * inverse * gain).astype(jnp.bfloat16)


def after(value, *others):
    return lax.optimization_barrier((value,) + others)[0]


def shift(value, perm):
    return lax.ppermute(value, "tensor", perm)


def gather_near(rows):
    return shift(rows, UP), shift(rows, DOWN)


def gather_far(near):
    half = near[0].shape[0] // 2
    return shift(near[0][:half], UP), shift(near[1][half:], DOWN)


def outgoing_rows(merged_in, image_counts, image_positions, rows_here, groups, tensor_devs):
    slots = image_positions.shape[0]
    live_slots = jnp.sum(image_counts) // 4
    usable = jnp.arange(slots, dtype=jnp.int32) < live_slots
    group = image_positions // (rows_here * tensor_devs)
    row = image_positions % rows_here
    mark = jnp.where(usable, row + 1, -1 - row).astype(jnp.bfloat16)
    order = jnp.arange(slots, dtype=jnp.int32)
    earlier = (group[:, None] == group[None, :]) & (order[:, None] < order[None, :])
    out_slot = group * (slots // groups) + jnp.sum(earlier.astype(jnp.int32), axis=0)
    chooser = (out_slot[None, :] == order[:, None]).astype(jnp.bfloat16)
    payload = jnp.concatenate([merged_in, jnp.broadcast_to(mark[:, None], (slots, 128))], axis=1)
    return jnp.dot(chooser, payload, preferred_element_type=jnp.float32).astype(jnp.bfloat16)


def project_body(owners, *refs):
    weight, bias, place, queries, keys, values, rows, total, sems = refs[-9:]
    pieces = refs[:-9]
    block = pl.program_id(0)
    step = weight.shape[0]
    owner_rows = place.shape[1]

    def copies(at):
        span = pl.ds(pl.multiple_of(at * step, step), step)
        lower = 0
        for index, piece in enumerate(pieces):
            height = piece.shape[0]
            yield pltpu.make_async_copy(piece.at[:, span], rows.at[pl.ds(lower, height), span], sems.at[at, index])
            lower += height

    @pl.when(block == 0)
    def _():
        for at in range(rows.shape[1] // step):
            for copy in copies(at):
                copy.start()

    for copy in copies(block):
        copy.wait()
    product = jnp.dot(
        rows[:, pl.ds(pl.multiple_of(block * step, step), step)], weight[...], preferred_element_type=jnp.float32
    )

    @pl.when(block == 0)
    def _():
        total[...] = product + bias[...]

    @pl.when(block > 0)
    def _():
        total[...] += product

    @pl.when(block == pl.num_programs(0) - 1)
    def _():
        wide = queries.shape[1]
        for owner in range(place.shape[0]):
            found = total[owner * owner_rows : (owner + 1) * owner_rows, :].astype(jnp.bfloat16)
            moved = jnp.dot(place[owner], found, preferred_element_type=jnp.float32).astype(jnp.bfloat16)
            at = pl.ds(pl.multiple_of(owners[owner] * owner_rows, owner_rows), owner_rows)
            queries[at, :] = moved[:, :wide]
            keys[at, :] = moved[:, wide : wide + HEAD_DIM]
            values[at, :] = moved[:, wide + HEAD_DIM :]


def project(owners, pieces, weight, bias, place):
    depth, width = weight.shape
    total_rows = sum(piece.shape[0] for piece in pieces)
    wide = width - 2 * HEAD_DIM
    outs = (wide, HEAD_DIM, HEAD_DIM)
    return pl.pallas_call(
        project_body,
        name="project",
        grid_spec=pltpu.PrefetchScalarGridSpec(
            num_scalar_prefetch=1,
            grid=(K_BLOCKS,),
            in_specs=[pl.BlockSpec(memory_space=pl.ANY)] * len(pieces)
            + [
                pl.BlockSpec((depth // K_BLOCKS, width), lambda k, o: (k, 0)),
                pl.BlockSpec((1, width), lambda k, o: (0, 0)),
                pl.BlockSpec(place.shape, lambda k, o: (0, 0, 0)),
            ],
            out_specs=[pl.BlockSpec((total_rows, columns), lambda k, o: (0, 0)) for columns in outs],
            scratch_shapes=[
                pltpu.VMEM((total_rows, depth), jnp.bfloat16),
                pltpu.VMEM((total_rows, width), jnp.float32),
                pltpu.SemaphoreType.DMA((K_BLOCKS, len(pieces))),
            ],
        ),
        out_shape=[jax.ShapeDtypeStruct((total_rows, columns), jnp.bfloat16) for columns in outs],
        compiler_params=pltpu.CompilerParams(
            dimension_semantics=("arbitrary",), vmem_limit_bytes=56 * 1024 * 1024
        ),
        cost_estimate=pl.CostEstimate(
            flops=2 * total_rows * depth * width, bytes_accessed=45_000_000, transcendentals=0
        ),
    )(owners, *pieces, weight, bias[None, :], place)


def shards(
    patches, ln_gain, ln_bias, fc1_weight, fc1_bias, fc2_weight, fc2_bias, image_counts, image_positions,
    text_embeds, keep_mask, norm_gain, qkv_weight, qkv_bias,
):
    groups = lax.axis_size("dp")
    tensor_devs = lax.axis_size("tensor")
    device = lax.axis_index("tensor")
    rows_here, _ = text_embeds.shape
    weight = lax.all_gather(qkv_weight, "dp", axis=0, tiled=True)

    patch_normed = layer_norm(patches, ln_gain, ln_bias).astype(jnp.bfloat16)
    merged_in = patch_normed.reshape(-1, 4 * patches.shape[1])
    slots, features = merged_in.shape
    outgoing = outgoing_rows(merged_in, image_counts, image_positions, rows_here, groups, tensor_devs)
    arrived = lax.all_to_all(
        outgoing.reshape(groups, slots // groups, -1), "dp", split_axis=0, concat_axis=0, tiled=True
    ).reshape(slots, -1)
    text_stream = (text_embeds.astype(jnp.float32) * keep_mask.astype(jnp.float32) * KEEP_SCALE).astype(jnp.bfloat16)
    text_normed = rms_norm(text_stream, norm_gain)
    arrived = after(arrived, text_normed)

    mark = arrived[:, features].astype(jnp.int32)
    own_row = jnp.abs(mark) - 1
    index = jnp.arange(rows_here, dtype=jnp.int32)
    lookup = own_row[:, None] == index[None, :]
    named = jnp.any(lookup, axis=0)
    rank = index - jnp.sum((own_row[:, None] < index[None, :]).astype(jnp.int32), axis=0)
    kept = rows_here - slots
    keep = (jnp.arange(kept, dtype=jnp.int32)[:, None] == rank[None, :]) & ~named[None, :]
    text_kept = jnp.dot(keep.astype(jnp.bfloat16), text_normed, preferred_element_type=jnp.float32).astype(jnp.bfloat16)

    near = gather_near(arrived)
    far = gather_far((after(near[0], text_kept), near[1]))
    mine = jnp.concatenate([arrived, *near, *far], axis=0)
    together = jnp.concatenate([mine, shift(mine, ACROSS)], axis=0)
    text_kept = after(text_kept, *far)
    x_near = gather_near(text_kept)

    product = jnp.dot(together[:, :features], fc1_weight, preferred_element_type=jnp.float32) + fc1_bias
    hidden = jax.nn.gelu(product, approximate=False).astype(jnp.bfloat16)
    for_other = jnp.dot(hidden[4 * slots :], fc2_weight, preferred_element_type=jnp.float32).astype(jnp.bfloat16)
    theirs = shift(for_other, ACROSS)
    partial = jnp.dot(hidden[: 4 * slots], fc2_weight, preferred_element_type=jnp.float32).astype(jnp.bfloat16)
    partial = lax.optimization_barrier(partial)
    paired = (partial.astype(jnp.float32) + theirs.astype(jnp.float32)).astype(jnp.bfloat16)
    half = slots // 2
    low = shift(paired[3 * slots : 3 * slots + half], UP)
    high = shift(paired[3 * slots + half : 4 * slots], DOWN)
    zeros = jnp.zeros_like(low)
    to_above = paired[2 * slots : 3 * slots].astype(jnp.float32) + jnp.concatenate([low, zeros], axis=0).astype(jnp.float32)
    to_below = paired[slots : 2 * slots].astype(jnp.float32) + jnp.concatenate([zeros, high], axis=0).astype(jnp.float32)
    from_below = shift(to_above.astype(jnp.bfloat16), UP)
    from_above = shift(to_below.astype(jnp.bfloat16), DOWN)
    summed = paired[:slots].astype(jnp.float32) + from_below.astype(jnp.float32) + from_above.astype(jnp.float32)
    tokens = (summed + fc2_bias).astype(jnp.bfloat16)

    token_mask = jnp.dot(
        lookup.astype(jnp.bfloat16), keep_mask.astype(jnp.bfloat16), preferred_element_type=jnp.float32
    )
    unused = jnp.dot(lookup.astype(jnp.bfloat16), text_stream, preferred_element_type=jnp.float32)
    token_stream = jnp.where(mark[:, None] > 0, tokens.astype(jnp.float32) * token_mask * KEEP_SCALE, unused)
    token_stream = token_stream.astype(jnp.bfloat16)
    token_normed = rms_norm(token_stream, norm_gain)
    t_near = gather_near(token_normed)
    landed = lax.dot_general(
        lookup.astype(jnp.bfloat16), token_stream, (((0,), (0,)), ((), ())), preferred_element_type=jnp.float32
    )
    stream = jnp.where(named[:, None], landed.astype(jnp.bfloat16), text_stream)

    slot_row = (jnp.abs(together[:, features].astype(jnp.int32)) - 1).reshape(tensor_devs, 1, slots)
    at_slot = slot_row == index[None, :, None]
    ranks = index[None, :] - jnp.sum((slot_row < index[None, :, None]).astype(jnp.int32), axis=2)
    at_kept = (ranks[:, :, None] == jnp.arange(kept, dtype=jnp.int32)) & ~jnp.any(at_slot, axis=2)[:, :, None]
    place = jnp.concatenate([at_kept, at_slot], axis=2).astype(jnp.bfloat16)
    owners = jnp.stack([(base + step) & 7 for base in (device, device ^ 1) for step in (0, -2, 2, 4)])
    owners = owners.astype(jnp.int32)

    x_far = gather_far((after(x_near[0], place, owners), x_near[1]))
    t_far = gather_far((after(t_near[0], stream), t_near[1]))
    pieces = [text_kept, token_normed, x_near[0], t_near[0], x_near[1], t_near[1], *x_far, *t_far]
    pieces = pieces + [shift(piece, ACROSS) for piece in pieces]
    queries, keys, values = project(owners, pieces, weight, qkv_bias, place)
    return (stream, queries, keys, values)


def solution(mesh):
    placed = (
        P(("dp", "tensor"), None), P(), P(), P(None, "tensor"), P("tensor"), P("tensor", None), P(),
        P(("dp", "tensor"), None), P(("dp", "tensor")), P(("dp", "tensor"), None), P(("dp", "tensor"), None),
        P(), P("dp", "tensor"), P("tensor"),
    )

    return jax.shard_map(
        shards, mesh=mesh, in_specs=placed,
        out_specs=(P(("dp", "tensor"), None), P("dp", "tensor"), P("dp", "tensor"), P("dp", "tensor")),
        check_vma=False,
    )
```

```python
import functools

import jax
import jax.numpy as jnp
from jax import lax
from jax.experimental import pallas as pl
from jax.experimental.pallas import tpu as pltpu
from jax.sharding import PartitionSpec as P


HEAD_DIM = 128
KEEP_SCALE = 1.0 / 0.9
K_BLOCKS = 8
TENSOR = 8

UP = [(t, (t + 2) % 8) for t in range(8)]
DOWN = [(t, (t - 2) % 8) for t in range(8)]
ACROSS = [(t, t ^ 1) for t in range(8)]


def rms_norm(inputs, gain):
    widened = inputs.astype(jnp.float32)
    inverse = lax.rsqrt(jnp.mean(widened * widened, axis=-1, keepdims=True) + 1e-06)
    return (widened * inverse * gain).astype(jnp.bfloat16)


def after(value, *others):
    return lax.optimization_barrier((value,) + others)[0]


def shift(value, perm):
    return lax.ppermute(value, "tensor", perm)


def gather_near(rows):
    return shift(rows, UP), shift(rows, DOWN)


def gather_far(near):
    half = near[0].shape[0] // 2
    return shift(near[0][:half], UP), shift(near[1][half:], DOWN)


def outgoing_body(rows_here, groups, counts, patches, gain, shift_by, positions, out):
    slots = out.shape[0]
    width = patches.shape[1]
    live = (counts[0, 0] + counts[0, 1] + counts[0, 2] + counts[0, 3]) // 4
    widened = patches[...].astype(jnp.float32)
    centered = widened - jnp.mean(widened, axis=-1, keepdims=True)
    spread = jnp.mean(centered * centered, axis=-1, keepdims=True)
    normed = (centered * lax.rsqrt(spread + 1e-06) * gain[...] + shift_by[...]).astype(jnp.bfloat16)

    first = lax.broadcasted_iota(jnp.int32, (slots, slots), 0)
    second = lax.broadcasted_iota(jnp.int32, (slots, slots), 1)
    position = jnp.broadcast_to(positions[...], (slots, slots))
    group = position // (rows_here * TENSOR)
    row = position % rows_here + 1
    mark = jnp.where(second < live, row, -row).astype(jnp.float32)
    own_group = jnp.sum(jnp.where(first == second, group, 0).astype(jnp.float32), axis=1, keepdims=True)
    earlier = (own_group == group.astype(jnp.float32)) & (first < second)
    rank = jnp.sum(earlier.astype(jnp.float32), axis=0, keepdims=True)
    chosen = group.astype(jnp.float32) * (slots // groups) + rank == first.astype(jnp.float32)
    source = jnp.sum(jnp.where(chosen, second, 0).astype(jnp.float32), axis=1, keepdims=True)
    marked = jnp.sum(jnp.where(chosen, mark, 0.0), axis=1, keepdims=True)
    patch = lax.broadcasted_iota(jnp.int32, (slots, patches.shape[0]), 1).astype(jnp.float32)
    for quarter in range(4):
        pick = (patch == 4.0 * source + quarter).astype(jnp.bfloat16)
        joined = jnp.dot(pick, normed, preferred_element_type=jnp.float32)
        out[:, quarter * width : (quarter + 1) * width] = joined.astype(jnp.bfloat16)
    out[:, 4 * width :] = jnp.broadcast_to(marked, (slots, 128)).astype(jnp.bfloat16)


def outgoing_rows(patches, gain, shift_by, image_counts, image_positions, rows_here, groups):
    slots = image_positions.shape[0]
    vmem = pl.BlockSpec(memory_space=pltpu.VMEM)
    return pl.pallas_call(
        functools.partial(outgoing_body, rows_here, groups),
        name="outgoing",
        in_specs=[pl.BlockSpec(memory_space=pltpu.SMEM), vmem, vmem, vmem, vmem],
        out_specs=vmem,
        out_shape=jax.ShapeDtypeStruct((slots, 4 * patches.shape[1] + 128), jnp.bfloat16),
        compiler_params=pltpu.CompilerParams(vmem_limit_bytes=16 * 1024 * 1024),
    )(image_counts, patches, gain[None, :], shift_by[None, :], image_positions[None, :])


def project_body(owners, *refs):
    weight, bias, place, queries, keys, values, rows, total, sems = refs[-9:]
    pieces = refs[:-9]
    block = pl.program_id(0)
    step = weight.shape[0]
    owner_rows = place.shape[1]

    def copies(at):
        span = pl.ds(pl.multiple_of(at * step, step), step)
        lower = 0
        for index, piece in enumerate(pieces):
            height = piece.shape[0]
            yield pltpu.make_async_copy(piece.at[:, span], rows.at[pl.ds(lower, height), span], sems.at[at, index])
            lower += height

    @pl.when(block == 0)
    def _():
        for at in range(rows.shape[1] // step):
            for copy in copies(at):
                copy.start()

    for copy in copies(block):
        copy.wait()

    @pl.when(block == 0)
    def _():
        total[...] = jnp.broadcast_to(bias[...], total.shape)

    span = pl.ds(pl.multiple_of(block * step, step), step)
    half = rows.shape[0] // 2
    for part in (slice(0, half), slice(half, 2 * half)):
        total[part, :] += jnp.dot(rows[part, span], weight[...], preferred_element_type=jnp.float32)

    @pl.when(block == pl.num_programs(0) - 1)
    def _():
        wide = queries.shape[1]
        for owner in range(place.shape[0]):
            found = total[owner * owner_rows : (owner + 1) * owner_rows, :].astype(jnp.bfloat16)
            moved = jnp.dot(place[owner], found, preferred_element_type=jnp.float32).astype(jnp.bfloat16)
            at = pl.ds(pl.multiple_of(owners[owner] * owner_rows, owner_rows), owner_rows)
            queries[at, :] = moved[:, :wide]
            keys[at, :] = moved[:, wide : wide + HEAD_DIM]
            values[at, :] = moved[:, wide + HEAD_DIM :]


def project(owners, pieces, weight, bias, place):
    depth, width = weight.shape
    total_rows = sum(piece.shape[0] for piece in pieces)
    wide = width - 2 * HEAD_DIM
    outs = (wide, HEAD_DIM, HEAD_DIM)
    return pl.pallas_call(
        project_body,
        name="project",
        grid_spec=pltpu.PrefetchScalarGridSpec(
            num_scalar_prefetch=1,
            grid=(K_BLOCKS,),
            in_specs=[pl.BlockSpec(memory_space=pl.ANY)] * len(pieces)
            + [
                pl.BlockSpec((depth // K_BLOCKS, width), lambda k, o: (k, 0)),
                pl.BlockSpec((1, width), lambda k, o: (0, 0)),
                pl.BlockSpec(place.shape, lambda k, o: (0, 0, 0)),
            ],
            out_specs=[pl.BlockSpec((total_rows, columns), lambda k, o: (0, 0)) for columns in outs],
            scratch_shapes=[
                pltpu.VMEM((total_rows, depth), jnp.bfloat16),
                pltpu.VMEM((total_rows, width), jnp.float32),
                pltpu.SemaphoreType.DMA((K_BLOCKS, len(pieces))),
            ],
        ),
        out_shape=[jax.ShapeDtypeStruct((total_rows, columns), jnp.bfloat16) for columns in outs],
        compiler_params=pltpu.CompilerParams(
            dimension_semantics=("arbitrary",), vmem_limit_bytes=56 * 1024 * 1024
        ),
        cost_estimate=pl.CostEstimate(
            flops=2 * total_rows * depth * width, bytes_accessed=45_000_000, transcendentals=0
        ),
    )(owners, *pieces, weight, bias[None, :], place)


def shards(
    patches, ln_gain, ln_bias, fc1_weight, fc1_bias, fc2_weight, fc2_bias, image_counts, image_positions,
    text_embeds, keep_mask, norm_gain, qkv_weight, qkv_bias,
):
    groups = lax.axis_size("dp")
    tensor_devs = lax.axis_size("tensor")
    device = lax.axis_index("tensor")
    rows_here, _ = text_embeds.shape
    weight = lax.all_gather(qkv_weight, "dp", axis=0, tiled=True)

    slots = image_positions.shape[0]
    features = 4 * patches.shape[1]
    outgoing = outgoing_rows(patches, ln_gain, ln_bias, image_counts, image_positions, rows_here, groups)
    arrived = lax.all_to_all(
        outgoing.reshape(groups, slots // groups, -1), "dp", split_axis=0, concat_axis=0, tiled=True
    ).reshape(slots, -1)
    text_stream = (text_embeds.astype(jnp.float32) * keep_mask.astype(jnp.float32) * KEEP_SCALE).astype(jnp.bfloat16)
    text_normed = rms_norm(text_stream, norm_gain)
    arrived = after(arrived, text_normed)

    mark = arrived[:, features].astype(jnp.int32)
    own_row = jnp.abs(mark) - 1
    index = jnp.arange(rows_here, dtype=jnp.int32)
    lookup = own_row[:, None] == index[None, :]
    named = jnp.any(lookup, axis=0)
    rank = index - jnp.sum((own_row[:, None] < index[None, :]).astype(jnp.int32), axis=0)
    kept = rows_here - slots
    keep = (jnp.arange(kept, dtype=jnp.int32)[:, None] == rank[None, :]) & ~named[None, :]
    text_kept = jnp.dot(keep.astype(jnp.bfloat16), text_normed, preferred_element_type=jnp.float32).astype(jnp.bfloat16)

    near = gather_near(arrived)
    far = gather_far((after(near[0], text_kept), near[1]))
    mine = jnp.concatenate([arrived, *near, *far], axis=0)
    together = jnp.concatenate([mine, shift(mine, ACROSS)], axis=0)
    text_kept = after(text_kept, *far)
    x_near = gather_near(text_kept)

    product = jnp.dot(together[:, :features], fc1_weight, preferred_element_type=jnp.float32) + fc1_bias
    hidden = jax.nn.gelu(product, approximate=False).astype(jnp.bfloat16)
    for_other = jnp.dot(hidden[4 * slots :], fc2_weight, preferred_element_type=jnp.float32).astype(jnp.bfloat16)
    theirs = shift(for_other, ACROSS)
    partial = jnp.dot(hidden[: 4 * slots], fc2_weight, preferred_element_type=jnp.float32).astype(jnp.bfloat16)
    partial = lax.optimization_barrier(partial)
    paired = (partial.astype(jnp.float32) + theirs.astype(jnp.float32)).astype(jnp.bfloat16)
    half = slots // 2
    low = shift(paired[3 * slots : 3 * slots + half], UP)
    high = shift(paired[3 * slots + half : 4 * slots], DOWN)
    zeros = jnp.zeros_like(low)
    to_above = paired[2 * slots : 3 * slots].astype(jnp.float32) + jnp.concatenate([low, zeros], axis=0).astype(jnp.float32)
    to_below = paired[slots : 2 * slots].astype(jnp.float32) + jnp.concatenate([zeros, high], axis=0).astype(jnp.float32)
    from_below = shift(to_above.astype(jnp.bfloat16), UP)
    from_above = shift(to_below.astype(jnp.bfloat16), DOWN)
    summed = paired[:slots].astype(jnp.float32) + from_below.astype(jnp.float32) + from_above.astype(jnp.float32)
    tokens = (summed + fc2_bias).astype(jnp.bfloat16)

    token_mask = jnp.dot(
        lookup.astype(jnp.bfloat16), keep_mask.astype(jnp.bfloat16), preferred_element_type=jnp.float32
    )
    unused = jnp.dot(lookup.astype(jnp.bfloat16), text_stream, preferred_element_type=jnp.float32)
    token_stream = jnp.where(mark[:, None] > 0, tokens.astype(jnp.float32) * token_mask * KEEP_SCALE, unused)
    token_stream = token_stream.astype(jnp.bfloat16)
    token_normed = rms_norm(token_stream, norm_gain)
    t_near = gather_near(token_normed)
    landed = lax.dot_general(
        lookup.astype(jnp.bfloat16), token_stream, (((0,), (0,)), ((), ())), preferred_element_type=jnp.float32
    )
    stream = jnp.where(named[:, None], landed.astype(jnp.bfloat16), text_stream)

    slot_row = (jnp.abs(together[:, features].astype(jnp.int32)) - 1).reshape(tensor_devs, 1, slots)
    at_slot = slot_row == index[None, :, None]
    ranks = index[None, :] - jnp.sum((slot_row < index[None, :, None]).astype(jnp.int32), axis=2)
    at_kept = (ranks[:, :, None] == jnp.arange(kept, dtype=jnp.int32)) & ~jnp.any(at_slot, axis=2)[:, :, None]
    place = jnp.concatenate([at_kept, at_slot], axis=2).astype(jnp.bfloat16)
    owners = jnp.stack([(base + step) & 7 for base in (device, device ^ 1) for step in (0, -2, 2, 4)])
    owners = owners.astype(jnp.int32)

    x_far = gather_far((after(x_near[0], place, owners), x_near[1]))
    early = [text_kept, *x_near, *x_far]
    crossed = [shift(piece, ACROSS) for piece in early]
    t_far = gather_far((after(t_near[0], stream, *crossed), t_near[1]))
    late = [token_normed, *t_near, *t_far]
    arrived_late = [shift(piece, ACROSS) for piece in late]
    pieces = []
    for kept_rows, slot_rows in ((early, late), (crossed, arrived_late)):
        for whole in range(3):
            pieces = pieces + [kept_rows[whole], slot_rows[whole]]
        pieces = pieces + kept_rows[3:] + slot_rows[3:]
    queries, keys, values = project(owners, pieces, weight, qkv_bias, place)
    return (stream, queries, keys, values)


def solution(mesh):
    placed = (
        P(("dp", "tensor"), None), P(), P(), P(None, "tensor"), P("tensor"), P("tensor", None), P(),
        P(("dp", "tensor"), None), P(("dp", "tensor")), P(("dp", "tensor"), None), P(("dp", "tensor"), None),
        P(), P("dp", "tensor"), P("tensor"),
    )

    return jax.shard_map(
        shards, mesh=mesh, in_specs=placed,
        out_specs=(P(("dp", "tensor"), None), P("dp", "tensor"), P("dp", "tensor"), P("dp", "tensor")),
        check_vma=False,
    )
```

```python
import functools

import jax
import jax.numpy as jnp
from jax import lax
from jax.experimental import pallas as pl
from jax.experimental.pallas import tpu as pltpu
from jax.sharding import PartitionSpec as P


HEAD_DIM = 128
KEEP_SCALE = 1.0 / 0.9
K_BLOCKS = 8
TENSOR = 8

UP = [(t, (t + 2) % 8) for t in range(8)]
DOWN = [(t, (t - 2) % 8) for t in range(8)]
ACROSS = [(t, t ^ 1) for t in range(8)]


def rms_norm(inputs, gain):
    widened = inputs.astype(jnp.float32)
    inverse = lax.rsqrt(jnp.mean(widened * widened, axis=-1, keepdims=True) + 1e-06)
    return (widened * inverse * gain).astype(jnp.bfloat16)


def after(value, *others):
    return lax.optimization_barrier((value,) + others)[0]


def shift(value, perm):
    return lax.ppermute(value, "tensor", perm)


def gather_near(rows):
    return shift(rows, UP), shift(rows, DOWN)


def gather_far(near):
    half = near[0].shape[0] // 2
    return shift(near[0][:half], UP), shift(near[1][half:], DOWN)


def outgoing_body(rows_here, groups, counts, patches, gain, shift_by, positions, out):
    slots = out.shape[0]
    width = patches.shape[1]
    live = (counts[0, 0] + counts[0, 1] + counts[0, 2] + counts[0, 3]) // 4
    widened = patches[...].astype(jnp.float32)
    centered = widened - jnp.mean(widened, axis=-1, keepdims=True)
    spread = jnp.mean(centered * centered, axis=-1, keepdims=True)
    normed = (centered * lax.rsqrt(spread + 1e-06) * gain[...] + shift_by[...]).astype(jnp.bfloat16)

    first = lax.broadcasted_iota(jnp.int32, (slots, slots), 0)
    second = lax.broadcasted_iota(jnp.int32, (slots, slots), 1)
    position = jnp.broadcast_to(positions[...], (slots, slots))
    group = position // (rows_here * TENSOR)
    row = position % rows_here + 1
    mark = jnp.where(second < live, row, -row).astype(jnp.float32)
    own_group = jnp.sum(jnp.where(first == second, group, 0).astype(jnp.float32), axis=1, keepdims=True)
    earlier = (own_group == group.astype(jnp.float32)) & (first < second)
    rank = jnp.sum(earlier.astype(jnp.float32), axis=0, keepdims=True)
    chosen = group.astype(jnp.float32) * (slots // groups) + rank == first.astype(jnp.float32)
    source = jnp.sum(jnp.where(chosen, second, 0).astype(jnp.float32), axis=1, keepdims=True)
    marked = jnp.sum(jnp.where(chosen, mark, 0.0), axis=1, keepdims=True)
    patch = lax.broadcasted_iota(jnp.int32, (slots, patches.shape[0]), 1).astype(jnp.float32)
    for quarter in range(4):
        pick = (patch == 4.0 * source + quarter).astype(jnp.bfloat16)
        joined = jnp.dot(pick, normed, preferred_element_type=jnp.float32)
        out[:, quarter * width : (quarter + 1) * width] = joined.astype(jnp.bfloat16)
    out[:, 4 * width :] = jnp.broadcast_to(marked, (slots, 128)).astype(jnp.bfloat16)


def outgoing_rows(patches, gain, shift_by, image_counts, image_positions, rows_here, groups):
    slots = image_positions.shape[0]
    vmem = pl.BlockSpec(memory_space=pltpu.VMEM)
    return pl.pallas_call(
        functools.partial(outgoing_body, rows_here, groups),
        name="outgoing",
        in_specs=[pl.BlockSpec(memory_space=pltpu.SMEM), vmem, vmem, vmem, vmem],
        out_specs=vmem,
        out_shape=jax.ShapeDtypeStruct((slots, 4 * patches.shape[1] + 128), jnp.bfloat16),
        compiler_params=pltpu.CompilerParams(vmem_limit_bytes=16 * 1024 * 1024),
    )(image_counts, patches, gain[None, :], shift_by[None, :], image_positions[None, :])


def project_body(owners, *refs):
    weight, bias, place, queries, keys, values, rows, total, sems = refs[-9:]
    pieces = refs[:-9]
    block = pl.program_id(0)
    step = weight.shape[0]
    owner_rows = place.shape[1]

    def copies(at):
        span = pl.ds(pl.multiple_of(at * step, step), step)
        lower = 0
        for index, piece in enumerate(pieces):
            height = piece.shape[0]
            yield pltpu.make_async_copy(piece.at[:, span], rows.at[pl.ds(lower, height), span], sems.at[at, index])
            lower += height

    @pl.when(block == 0)
    def _():
        for at in range(rows.shape[1] // step):
            for copy in copies(at):
                copy.start()

    for copy in copies(block):
        copy.wait()

    @pl.when(block == 0)
    def _():
        total[...] = jnp.broadcast_to(bias[...], total.shape)

    span = pl.ds(pl.multiple_of(block * step, step), step)
    half = rows.shape[0] // 2
    for part in (slice(0, half), slice(half, 2 * half)):
        total[part, :] += jnp.dot(rows[part, span], weight[...], preferred_element_type=jnp.float32)

    @pl.when(block == pl.num_programs(0) - 1)
    def _():
        wide = queries.shape[1]
        for owner in range(place.shape[0]):
            found = total[owner * owner_rows : (owner + 1) * owner_rows, :].astype(jnp.bfloat16)
            moved = jnp.dot(place[owner], found, preferred_element_type=jnp.float32).astype(jnp.bfloat16)
            at = pl.ds(pl.multiple_of(owners[owner] * owner_rows, owner_rows), owner_rows)
            queries[at, :] = moved[:, :wide]
            keys[at, :] = moved[:, wide : wide + HEAD_DIM]
            values[at, :] = moved[:, wide + HEAD_DIM :]


def project(owners, pieces, weight, bias, place):
    depth, width = weight.shape
    total_rows = sum(piece.shape[0] for piece in pieces)
    wide = width - 2 * HEAD_DIM
    outs = (wide, HEAD_DIM, HEAD_DIM)
    return pl.pallas_call(
        project_body,
        name="project",
        grid_spec=pltpu.PrefetchScalarGridSpec(
            num_scalar_prefetch=1,
            grid=(K_BLOCKS,),
            in_specs=[pl.BlockSpec(memory_space=pl.ANY)] * len(pieces)
            + [
                pl.BlockSpec((depth // K_BLOCKS, width), lambda k, o: (k, 0)),
                pl.BlockSpec((1, width), lambda k, o: (0, 0)),
                pl.BlockSpec(place.shape, lambda k, o: (0, 0, 0)),
            ],
            out_specs=[pl.BlockSpec((total_rows, columns), lambda k, o: (0, 0)) for columns in outs],
            scratch_shapes=[
                pltpu.VMEM((total_rows, depth), jnp.bfloat16),
                pltpu.VMEM((total_rows, width), jnp.float32),
                pltpu.SemaphoreType.DMA((K_BLOCKS, len(pieces))),
            ],
        ),
        out_shape=[jax.ShapeDtypeStruct((total_rows, columns), jnp.bfloat16) for columns in outs],
        compiler_params=pltpu.CompilerParams(
            dimension_semantics=("arbitrary",), vmem_limit_bytes=56 * 1024 * 1024
        ),
        cost_estimate=pl.CostEstimate(
            flops=2 * total_rows * depth * width, bytes_accessed=45_000_000, transcendentals=0
        ),
    )(owners, *pieces, weight, bias, place)


def shards(
    patches, ln_gain, ln_bias, fc1_weight, fc1_bias, fc2_weight, fc2_bias, image_counts, image_positions,
    text_embeds, keep_mask, norm_gain, qkv_weight, qkv_bias,
):
    groups = lax.axis_size("dp")
    tensor_devs = lax.axis_size("tensor")
    device = lax.axis_index("tensor")
    rows_here, _ = text_embeds.shape
    weight = lax.all_gather(qkv_weight, "dp", axis=0, tiled=True)

    slots = image_positions.shape[0]
    features = 4 * patches.shape[1]
    outgoing = outgoing_rows(patches, ln_gain, ln_bias, image_counts, image_positions, rows_here, groups)
    arrived = lax.all_to_all(
        outgoing.reshape(groups, slots // groups, -1), "dp", split_axis=0, concat_axis=0, tiled=True
    ).reshape(slots, -1)
    text_stream = (text_embeds.astype(jnp.float32) * keep_mask.astype(jnp.float32) * KEEP_SCALE).astype(jnp.bfloat16)
    text_normed = rms_norm(text_stream, norm_gain)
    arrived = after(arrived, text_normed)

    mark = arrived[:, features].astype(jnp.int32)
    own_row = jnp.abs(mark) - 1
    index = jnp.arange(rows_here, dtype=jnp.int32)
    lookup = own_row[:, None] == index[None, :]
    named = jnp.any(lookup, axis=0)
    rank = index - jnp.sum((own_row[:, None] < index[None, :]).astype(jnp.int32), axis=0)
    kept = rows_here - slots
    keep = (jnp.arange(kept, dtype=jnp.int32)[:, None] == rank[None, :]) & ~named[None, :]
    text_kept = jnp.dot(keep.astype(jnp.bfloat16), text_normed, preferred_element_type=jnp.float32).astype(jnp.bfloat16)

    near = gather_near(arrived)
    far = gather_far((after(near[0], text_kept), near[1]))
    mine = jnp.concatenate([arrived, *near, *far], axis=0)
    together = jnp.concatenate([mine, shift(mine, ACROSS)], axis=0)
    text_kept = after(text_kept, *far)
    x_near = gather_near(text_kept)

    product = jnp.dot(together[:, :features], fc1_weight, preferred_element_type=jnp.float32) + fc1_bias
    hidden = jax.nn.gelu(product, approximate=False).astype(jnp.bfloat16)
    for_other = jnp.dot(hidden[4 * slots :], fc2_weight, preferred_element_type=jnp.float32).astype(jnp.bfloat16)
    theirs = shift(for_other, ACROSS)
    partial = jnp.dot(hidden[: 4 * slots], fc2_weight, preferred_element_type=jnp.float32).astype(jnp.bfloat16)
    partial = lax.optimization_barrier(partial)
    paired = (partial.astype(jnp.float32) + theirs.astype(jnp.float32)).astype(jnp.bfloat16)
    half = slots // 2
    low = shift(paired[3 * slots : 3 * slots + half], UP)
    high = shift(paired[3 * slots + half : 4 * slots], DOWN)
    zeros = jnp.zeros_like(low)
    to_above = paired[2 * slots : 3 * slots].astype(jnp.float32) + jnp.concatenate([low, zeros], axis=0).astype(jnp.float32)
    to_below = paired[slots : 2 * slots].astype(jnp.float32) + jnp.concatenate([zeros, high], axis=0).astype(jnp.float32)
    from_below = shift(to_above.astype(jnp.bfloat16), UP)
    from_above = shift(to_below.astype(jnp.bfloat16), DOWN)
    summed = paired[:slots].astype(jnp.float32) + from_below.astype(jnp.float32) + from_above.astype(jnp.float32)
    tokens = (summed + fc2_bias).astype(jnp.bfloat16)

    token_mask = jnp.dot(
        lookup.astype(jnp.bfloat16), keep_mask.astype(jnp.bfloat16), preferred_element_type=jnp.float32
    )
    unused = jnp.dot(lookup.astype(jnp.bfloat16), text_stream, preferred_element_type=jnp.float32)
    token_stream = jnp.where(mark[:, None] > 0, tokens.astype(jnp.float32) * token_mask * KEEP_SCALE, unused)
    token_stream = token_stream.astype(jnp.bfloat16)
    token_normed = rms_norm(token_stream, norm_gain)
    t_near = gather_near(token_normed)
    landed = lax.dot_general(
        lookup.astype(jnp.bfloat16), token_stream, (((0,), (0,)), ((), ())), preferred_element_type=jnp.float32
    )
    stream = jnp.where(named[:, None], landed.astype(jnp.bfloat16), text_stream)

    slot_row = (jnp.abs(together[:, features].astype(jnp.int32)) - 1).reshape(tensor_devs, 1, slots)
    at_slot = slot_row == index[None, :, None]
    ranks = index[None, :] - jnp.sum((slot_row < index[None, :, None]).astype(jnp.int32), axis=2)
    at_kept = (ranks[:, :, None] == jnp.arange(kept, dtype=jnp.int32)) & ~jnp.any(at_slot, axis=2)[:, :, None]
    place = jnp.concatenate([at_kept, at_slot], axis=2).astype(jnp.bfloat16)
    owners = jnp.stack([(base + step) & 7 for base in (device, device ^ 1) for step in (0, -2, 2, 4)])
    owners = owners.astype(jnp.int32)

    bias = qkv_bias[None, :]
    x_far = gather_far((after(x_near[0], place, owners, bias), x_near[1]))
    early = [text_kept, *x_near, *x_far]
    crossed = [shift(piece, ACROSS) for piece in early]
    t_far = gather_far((after(t_near[0], *crossed), t_near[1]))
    late = [token_normed, *t_near, *t_far]
    arrived_late = [shift(piece, ACROSS) for piece in late[:3]]
    last = after(t_far[0], stream, *arrived_late), after(t_far[1], stream, *arrived_late)
    arrived_late = arrived_late + [shift(piece, ACROSS) for piece in last]
    pieces = []
    for kept_rows, slot_rows in ((early, late), (crossed, arrived_late)):
        for whole in range(3):
            pieces = pieces + [kept_rows[whole], slot_rows[whole]]
        pieces = pieces + kept_rows[3:] + slot_rows[3:]
    queries, keys, values = project(owners, pieces, weight, bias, place)
    return (stream, queries, keys, values)


def solution(mesh):
    placed = (
        P(("dp", "tensor"), None), P(), P(), P(None, "tensor"), P("tensor"), P("tensor", None), P(),
        P(("dp", "tensor"), None), P(("dp", "tensor")), P(("dp", "tensor"), None), P(("dp", "tensor"), None),
        P(), P("dp", "tensor"), P("tensor"),
    )

    return jax.shard_map(
        shards, mesh=mesh, in_specs=placed,
        out_specs=(P(("dp", "tensor"), None), P("dp", "tensor"), P("dp", "tensor"), P("dp", "tensor")),
        check_vma=False,
    )
```
